64 devices in a mesh: rep: 4 (over x, y), dp: 16 (over z, core).
Axes of the slice: x: 2, y: 2, z: 8, core: 2. Of those that a mesh axis runs over, the one named last changes fastest.
The devices are a block of a 4x4x8 slice.
Arguments:
- x: bfloat16 [64, 2048, 640], P(('rep', 'dp')), parts along dimension 0
- dy: bfloat16 [64, 2048, 640], P(('rep', 'dp')), parts along dimension 0
- w_gate: bfloat16 [2, 640, 2048], replicated
- w_up: bfloat16 [2, 640, 2048], replicated
- w_down: bfloat16 [2, 2048, 640], replicated
- m_w_gate: float32 [2, 640, 2048], replicated
- m_w_up: float32 [2, 640, 2048], replicated
- m_w_down: float32 [2, 2048, 640], replicated
- v_w_gate: float32 [2, 640, 2048], replicated
- v_w_up: float32 [2, 640, 2048], replicated
- v_w_down: float32 [2, 2048, 640], replicated
Outputs:
- output 1: bfloat16 [8, 640, 2048], P('rep'), parts along dimension 0
- output 2: bfloat16 [8, 640, 2048], P('rep'), parts along dimension 0
- output 3: bfloat16 [8, 2048, 640], P('rep'), parts along dimension 0
- output 4: float32 [8, 640, 2048], P('rep'), parts along dimension 0
- output 5: float32 [8, 640, 2048], P('rep'), parts along dimension 0
- output 6: float32 [8, 2048, 640], P('rep'), parts along dimension 0
- output 7: float32 [8, 640, 2048], P('rep'), parts along dimension 0
- output 8: float32 [8, 640, 2048], P('rep'), parts along dimension 0
- output 9: float32 [8, 2048, 640], P('rep'), parts along dimension 0
There are 4 independent parts. The reference program is written for one: setup_inputs(seed, part) draws one part's arguments, and reference() takes and returns one part's arrays. A program takes and returns all parts, laid end to end along the dimension named above; an argument that names none is the same for every part.
All inputs are finite; a program needn't handle non-finite values.
Results may differ from the reference program's by a relative error of at most 0.0226.
Values are sent between devices in bfloat16 or wider.
A program may use at most 768 MiB of HBM per device.

```python
import jax
import jax.numpy as jnp
from jax import lax

SEQUENCES = 16
TOKENS = 2048
D = 640
FF = 2048
LAYERS = 2
NAMES = ("w_gate", "w_up", "w_down")
SHAPES = {"w_gate": (LAYERS, D, FF), "w_up": (LAYERS, D, FF), "w_down": (LAYERS, FF, D)}


def bump(key, n, height):
    away = (jnp.arange(n, dtype=jnp.int32) - jax.random.randint(key, (), 0, n, jnp.int32)) % n
    return jnp.where(away < n // 8, height, 1.0)


def together(key, own, strength):
    shared = jax.random.normal(key, own.shape[1:], jnp.float32)
    return (own + strength * shared) * lax.rsqrt(1 + strength * strength)


def setup_inputs(seed: int = 0, part: int = 0) -> dict:
    kx, kdy, ka, kb, kz, kf, kh, kl, *keys = jax.random.split(jax.random.key(seed), 8 + 3 * len(NAMES))
    kx, kdy, ka, kb = (jax.random.fold_in(k, part) for k in (kx, kdy, ka, kb))
    kw, km, kv = (keys[i::3] for i in range(3))
    shape = (SEQUENCES, TOKENS, D)
    much_x, much_dy = jax.random.uniform(kz, (2,), jnp.float32, 0.0, 1.0)
    loud = 2.0 ** jax.random.uniform(jax.random.fold_in(kz, 1), (), jnp.float32, -1.0, 2.0)
    layers = 2.0 ** jax.random.uniform(kl, (LAYERS, 1, 1), jnp.float32, -1.0, 1.0)
    x = together(ka, jax.random.normal(kx, shape, jnp.float32), much_x) * bump(kf, D, 4.0)
    dy = together(kb, jax.random.normal(kdy, shape, jnp.float32), much_dy)
    drawn = {"x": x.astype(jnp.bfloat16), "dy": (loud * dy * (SEQUENCES * TOKENS) ** -0.5).astype(jnp.bfloat16)}
    for key, name in zip(kw, NAMES, strict=True):
        w = jax.random.normal(key, SHAPES[name], jnp.float32) * SHAPES[name][1] ** -0.5
        drawn[name] = (w * {"w_gate": 1.0, "w_up": bump(kh, FF, 4.0), "w_down": layers}[name]).astype(jnp.bfloat16)
    for key, name in zip(km, NAMES, strict=True):
        drawn[f"m_{name}"] = 0.1 * jax.random.normal(key, SHAPES[name], jnp.float32)
    for key, name in zip(kv, NAMES, strict=True):
        drawn[f"v_{name}"] = jax.random.uniform(key, SHAPES[name], jnp.float32, 0.005, 0.015)
    return drawn


def matmul(a, w):
    return jnp.dot(a, w, preferred_element_type=jnp.float32).astype(jnp.bfloat16)


def normed(h):
    wide = h.astype(jnp.float32)
    scale = lax.rsqrt(jnp.mean(wide**2, -1, keepdims=True) + 1e-6)
    return (wide * scale).astype(jnp.bfloat16)


def layer(h, w):
    a = normed(h)
    gate = jnp.dot(a, w["w_gate"], preferred_element_type=jnp.float32)
    up = jnp.dot(a, w["w_up"], preferred_element_type=jnp.float32)
    return h + matmul((jax.nn.silu(gate) * up).astype(jnp.bfloat16), w["w_down"])


def adamw(w, m, v, g):
    m = 0.9 * m + 0.1 * g
    v = 0.95 * v + 0.05 * g * g
    step = m * lax.rsqrt(v + 1e-8) + 0.1 * w
    return (w - 0.02 * step).astype(jnp.bfloat16), m, v


def clipped(gradients, sum_of_squares, count):
    factor = jnp.minimum(1.0, 0.5 * lax.rsqrt(sum_of_squares / count + 1e-30))
    return [g * factor for g in gradients]


def stack(weights, h):
    return lax.scan(lambda h, w: (layer(h, w), None), h, weights)[0]


def reference(x, dy, w_gate, w_up, w_down, m_w_gate, m_w_up, m_w_down, v_w_gate, v_w_up, v_w_down):
    weights = dict(zip(NAMES, (w_gate, w_up, w_down), strict=True))

    def take(so_far, sequence):
        h, by_y = sequence
        _, back = jax.vjp(lambda w: stack(w, h), weights)
        return jax.tree.map(lambda total, term: total + term.astype(jnp.float32), so_far, back(by_y)[0]), None

    none_yet = {name: jnp.zeros(w.shape, jnp.float32) for name, w in weights.items()}
    by_weights, _ = lax.scan(take, none_yet, (x, dy))
    gradients = [by_weights[name].astype(jnp.bfloat16).astype(jnp.float32) for name in NAMES]
    gradients = clipped(gradients, sum(jnp.sum(g * g) for g in gradients), sum(g.size for g in gradients))
    new = [
        adamw(w.astype(jnp.float32), m, v, g)
        for w, m, v, g in zip((w_gate, w_up, w_down), (m_w_gate, m_w_up, m_w_down), (v_w_gate, v_w_up, v_w_down), gradients, strict=True)
    ]
    return tuple(one[which] for which in range(3) for one in new)
```

```python
import functools

import jax
import jax.numpy as jnp
from jax import lax
from jax.experimental import pallas as pl
from jax.experimental.pallas import tpu as pltpu
from jax.sharding import PartitionSpec as P

MESH = pl.DeviceIdType.MESH
F32, BF16 = jnp.float32, jnp.bfloat16
HBM = pl.BlockSpec(memory_space=pltpu.HBM)
BLOCK = 256
LANES = 128
ROWS = 256
VMEM_LIMIT = 66 * 1024 * 1024 - 4 * 1024 * 1024


def sigmoid(x):
    return 0.5 * jnp.tanh(0.5 * x) + 0.5


def dot(a, b, contract=((1,), (0,))):
    return lax.dot_general(a, b, (contract, ((), ())), preferred_element_type=F32)


def scale_of(wide):
    return lax.rsqrt(jnp.mean(wide * wide, -1, keepdims=True) + 1e-6)


def normed(h):
    wide = h.astype(F32)
    return (wide * scale_of(wide)).astype(BF16)


def forward_kernel(x_ref, dy_ref, wg_ref, wu_ref, wd_ref, h_ref, a_ref, at_ref, dyt_ref, act_ref):
    x = x_ref[...]
    a = normed(x)
    a_ref[0] = a
    at_ref[0] = a.T
    dyt_ref[...] = dy_ref[...].T
    width = 2 * BLOCK
    for f in range(0, act_ref.shape[1], width):
        gate = dot(a, wg_ref[0, :, f : f + width])
        up = dot(a, wu_ref[0, :, f : f + width])
        act_ref[:, f : f + width] = (gate * sigmoid(gate) * up).astype(BF16)
    h = x + dot(act_ref[...], wd_ref[0]).astype(BF16)
    h_ref[...] = h
    b = normed(h)
    a_ref[1] = b
    at_ref[1] = b.T


def forward(x, dy, wg, wu, wd):
    tokens, d = x.shape
    ff = wg.shape[2]
    rows = min(512, tokens)
    tile = pl.BlockSpec((rows, d), lambda i: (i, 0))
    return pl.pallas_call(
        forward_kernel,
        grid=(tokens // rows,),
        in_specs=[tile, tile]
        + [pl.BlockSpec((1, d, ff), lambda i: (0, 0, 0))] * 2
        + [pl.BlockSpec((1, ff, d), lambda i: (0, 0, 0))],
        out_specs=[
            tile,
            pl.BlockSpec((2, rows, d), lambda i: (0, i, 0)),
            pl.BlockSpec((2, d, rows), lambda i: (0, 0, i)),
            pl.BlockSpec((d, rows), lambda i: (0, i)),
        ],
        out_shape=[
            jax.ShapeDtypeStruct((tokens, d), BF16),
            jax.ShapeDtypeStruct((2, tokens, d), BF16),
            jax.ShapeDtypeStruct((2, d, tokens), BF16),
            jax.ShapeDtypeStruct((d, tokens), BF16),
        ],
        scratch_shapes=[pltpu.VMEM((rows, ff), BF16)],
        compiler_params=pltpu.CompilerParams(vmem_limit_bytes=VMEM_LIMIT),
    )(x, dy, wg, wu, wd)


def backward_kernel(
    chips, a_hbm, at_hbm, dy_hbm, dyt_hbm, h_hbm, wg_hbm, wu_hbm, wd_hbm, sums,
    a_ref, at_ref, dy_ref, dyt_ref, h_ref, wg_ref, wu_ref, wd_ref, p_ref, dg_ref, du_ref, dag_ref, dau_ref,
    own_ref, got_ref, both_ref, land_ref,
    load_sem, w_sem, pair_send, pair_recv, rs_send, rs_recv, ag_send, ag_recv, share_send, share_recv, keep_sem,
):
    layers, tokens, d = a_ref.shape
    ff = wg_hbm.shape[2]
    per_layer = ff // BLOCK
    blocks = layers * per_layer
    chunk = 3 * d // chips
    tiles = tokens // ROWS
    first_tiles = tiles * 3 // 4

    me = lax.axis_index("dp")
    z, core = me // 2, me % 2
    other = 1 - core
    partner = {"dp": z * 2 + other}

    def along(step):
        return {"dp": lax.rem(z + step + chips, chips) * 2 + core}

    def rows_of(c):
        return pl.ds(pl.multiple_of(c * chunk, chunk), chunk)

    def weights(t, slot):
        layer = layers - 1 - t // per_layer
        f = pl.multiple_of(lax.rem(t, per_layer) * BLOCK, BLOCK)
        return [
            pltpu.make_async_copy(wg_hbm.at[layer, :, pl.ds(f, BLOCK)], wg_ref.at[slot], w_sem.at[slot, 0]),
            pltpu.make_async_copy(wu_hbm.at[layer, :, pl.ds(f, BLOCK)], wu_ref.at[slot], w_sem.at[slot, 1]),
            pltpu.make_async_copy(wd_hbm.at[layer, pl.ds(f, BLOCK), :], wd_ref.at[slot], w_sem.at[slot, 2]),
        ]

    last = layers - 1
    loads = [
        pltpu.make_async_copy(a_hbm.at[last], a_ref.at[last], load_sem.at[0]),
        pltpu.make_async_copy(dy_hbm, dy_ref, load_sem.at[1]),
        pltpu.make_async_copy(at_hbm.at[last], at_ref.at[last], load_sem.at[2]),
        pltpu.make_async_copy(dyt_hbm, dyt_ref, load_sem.at[3]),
        pltpu.make_async_copy(h_hbm, h_ref, load_sem.at[4]),
        pltpu.make_async_copy(a_hbm.at[0], a_ref.at[0], load_sem.at[5]),
        pltpu.make_async_copy(at_hbm.at[0], at_ref.at[0], load_sem.at[6]),
    ]
    loads[0].start()
    for copy in weights(0, 0):
        copy.start()
    for copy in loads[1:]:
        copy.start()

    barrier = pltpu.get_barrier_semaphore()
    for peer in (partner, along(1), along(-1)):
        pl.semaphore_signal(barrier, inc=1, device_id=peer, device_id_type=MESH)
    pl.semaphore_wait(barrier, 3)

    def pair_copy(b):
        slot = lax.rem(b, 2)
        return pltpu.make_async_remote_copy(
            own_ref.at[slot, other], got_ref.at[slot], pair_send.at[slot], pair_recv.at[slot], partner, MESH
        )

    def rs_copy(b, s):
        way = 1 - 2 * lax.rem(b, 2)
        return pltpu.make_async_remote_copy(
            land_ref.at[b, s - 1], land_ref.at[b, s], rs_send.at[b, s - 1], rs_recv.at[b, s - 1], along(way), MESH
        )

    def ag_copy(src, b, c, side, hop):
        way = (1 - 2 * lax.rem(b, 2)) * (1 - 2 * side)
        place = side * (chips // 2) + hop - 1
        return pltpu.make_async_remote_copy(
            src, sums.at[b, core, rows_of(c), :], ag_send.at[b, place], ag_recv.at[b, place], along(way), MESH
        )

    def share_copy(src, b, c):
        return pltpu.make_async_remote_copy(src, sums.at[b, core, rows_of(c), :], share_send, share_recv, partner, MESH)

    def keep_copy(b):
        return pltpu.make_async_copy(land_ref.at[b, chips - 1], sums.at[b, core, rows_of(z), :], keep_sem.at[b])

    hops = (chips // 2, chips - 1 - chips // 2)

    def tick(u, odd):
        if not odd:
            b = u - 1

            @pl.when((b >= 0) & (b < blocks))
            def _():
                slot = lax.rem(b, 2)
                pair_copy(b).wait()

                def add(i, _):
                    r = pl.ds(pl.multiple_of(i * chunk, chunk), chunk)
                    both_ref[lax.rem(b, 4), r] = own_ref[slot, core, r].astype(F32) + got_ref[slot, r].astype(F32)
                    return 0

                lax.fori_loop(0, chips, add, 0)

        steps = [s for s in range(chips, 0, -1) if (s + odd) % 2 == 1]
        for s in steps:
            b = u - (s + 1) // 2 if not odd else u - s // 2

            @pl.when((b >= 0) & (b < blocks))
            def _(s=s, b=b):
                way = 1 - 2 * lax.rem(b, 2)
                term = both_ref[lax.rem(b, 4), rows_of(lax.rem(z - way * s + 2 * chips, chips))]
                if s > 1:
                    rs_copy(b, s - 1).wait_recv()
                    term = term + land_ref[b, s - 1].astype(F32)
                land_ref[b, s - 1] = term.astype(BF16)

        for s in steps:
            b = u - (s + 1) // 2 if not odd else u - s // 2

            @pl.when((b >= 0) & (b < blocks))
            def _(s=s, b=b):
                if s < chips:
                    rs_copy(b, s).start()
                else:
                    src = land_ref.at[b, chips - 1]
                    for side in range(2):
                        ag_copy(src, b, z, side, 1).start()
                    share_copy(src, b, z).start()
                    keep_copy(b).start()

        for hop in range(1, hops[0] + 1):
            if (chips + 1 + hop + odd) % 2:
                continue
            b = u - (chips + 1 + hop - odd) // 2

            @pl.when((b >= 0) & (b < blocks))
            def _(hop=hop, b=b):
                for side in range(2):
                    if hop > hops[side]:
                        continue
                    way = (1 - 2 * lax.rem(b, 2)) * (1 - 2 * side)
                    c = lax.rem(z - way * hop + 2 * chips, chips)
                    ag_copy(sums.at[b, core, rows_of(c), :], b, c, side, hop).wait_recv()
                    if hop < hops[side]:
                        ag_copy(sums.at[b, core, rows_of(c), :], b, c, side, hop + 1).start()
                    share_copy(sums.at[b, core, rows_of(c), :], b, c).start()

    def token_tile(t, layer, slot, i):
        r = pl.ds(pl.multiple_of(i * ROWS, ROWS), ROWS)
        a = a_ref[layer, r]
        wg, wu = wg_ref[slot], wu_ref[slot]
        gate, up = dot(a, wg), dot(a, wu)
        by_p = dot(dy_ref[r], wd_ref[slot], ((1,), (1,))).astype(BF16).astype(F32)
        s = sigmoid(gate)
        silu = gate * s
        p_ref[r] = (silu * up).astype(BF16)
        by_up = (by_p * silu).astype(BF16)
        by_gate = (by_p * up * (s + silu * (1.0 - s))).astype(BF16)
        dg_ref[r] = by_gate
        du_ref[r] = by_up

        @pl.when(layer > 0)
        def _():
            by_g, by_u = dot(by_gate, wg, ((1,), (1,))), dot(by_up, wu, ((1,), (1,)))
            start = lax.rem(t, per_layer) == 0

            @pl.when(start)
            def _():
                dag_ref[r] = by_g
                dau_ref[r] = by_u

            @pl.when(jnp.logical_not(start))
            def _():
                dag_ref[r] += by_g
                dau_ref[r] += by_u

    def next_layer(i, _):
        r = pl.ds(pl.multiple_of(i * ROWS, ROWS), ROWS)
        wide = h_ref[r].astype(F32)
        by_a = (dag_ref[r].astype(BF16).astype(F32) + dau_ref[r].astype(BF16).astype(F32)).astype(BF16).astype(F32)
        scale = scale_of(wide)
        inner = jnp.sum(by_a * wide, -1, keepdims=True) * (scale * scale * scale / d)
        by_h = dy_ref[r] + (by_a * scale - wide * inner).astype(BF16)
        dy_ref[r] = by_h
        dyt_ref[:, r] = by_h.T
        return 0

    def block(t, _):
        slot = lax.rem(t, 2)
        layer = layers - 1 - t // per_layer

        @pl.when(t + 1 < blocks)
        def _():
            for copy in weights(t + 1, 1 - slot):
                copy.start()

        @pl.when(t == 0)
        def _():
            loads[0].wait()
            loads[1].wait()

        @pl.when(t == per_layer)
        def _():
            for copy in loads[4:]:
                copy.wait()
            lax.fori_loop(0, tiles, next_layer, 0)

        for copy in weights(t, slot):
            copy.wait()

        def some(i, _):
            token_tile(t, layer, slot, i)
            return 0

        lax.fori_loop(0, first_tiles, some, 0)
        tick(t, 0)
        lax.fori_loop(first_tiles, tiles, some, 0)

        @pl.when(t == 0)
        def _():
            loads[2].wait()
            loads[3].wait()

        for place, (left, right) in enumerate(
            ((at_ref.at[layer], dg_ref), (at_ref.at[layer], du_ref), (dyt_ref, p_ref))
        ):
            g = dot(left[...], right[...]).astype(BF16)
            for half in range(2):
                own_ref[slot, half, place * d : (place + 1) * d, :] = g[:, half * LANES : (half + 1) * LANES]
        tick(t, 1)
        pair_copy(t).start()
        return 0

    lax.fori_loop(0, blocks, block, 0)

    def drain(u, _):
        tick(u, 0)
        tick(u, 1)
        return 0

    lax.fori_loop(blocks, (2 * (blocks - 1) + chips + 1 + hops[0]) // 2 + 1, drain, 0)

    def finish(b, _):
        for s in range(1, chips):
            rs_copy(b, s).wait_send()
        for side in range(2):
            for hop in range(1, hops[side] + 1):
                ag_copy(land_ref.at[b, chips - 1], b, z, side, hop).wait_send()
        keep_copy(b).wait()
        return 0

    lax.fori_loop(0, blocks, finish, 0)
    pltpu.make_async_copy(sums.at[:, core], sums.at[:, core], share_send).wait()
    pltpu.make_async_copy(sums.at[:, other], sums.at[:, other], share_recv).wait()


def backward(chips, a, at, dy, dyt, h, wg, wu, wd):
    layers, tokens, d = a.shape
    ff = wg.shape[2]
    blocks = layers * ff // BLOCK
    chunk = 3 * d // chips
    vmem = pltpu.VMEM
    sem = pltpu.SemaphoreType.DMA
    flops = 2 * tokens * d * ff * (6 * layers + 2)
    return pl.pallas_call(
        functools.partial(backward_kernel, chips),
        out_shape=jax.ShapeDtypeStruct((blocks, 2, 3 * d, LANES), BF16),
        in_specs=[HBM] * 8,
        out_specs=HBM,
        scratch_shapes=[
            vmem((layers, tokens, d), BF16), vmem((layers, d, tokens), BF16), vmem((tokens, d), BF16), vmem((d, tokens), BF16),
            vmem((tokens, d), BF16), vmem((2, d, BLOCK), BF16), vmem((2, d, BLOCK), BF16), vmem((2, BLOCK, d), BF16),
            vmem((tokens, BLOCK), BF16), vmem((tokens, BLOCK), BF16), vmem((tokens, BLOCK), BF16),
            vmem((tokens, d), F32), vmem((tokens, d), F32),
            vmem((2, 2, 3 * d, LANES), BF16), vmem((2, 3 * d, LANES), BF16), vmem((4, 3 * d, LANES), F32),
            vmem((blocks, chips, chunk, LANES), BF16),
            sem((7,)), sem((2, 3)), sem((2,)), sem((2,)), sem((blocks, chips - 1)), sem((blocks, chips - 1)),
            sem((blocks, chips - 1)), sem((blocks, chips - 1)), sem, sem, sem((blocks,)),
        ],
        compiler_params=pltpu.CompilerParams(collective_id=0, has_side_effects=True, vmem_limit_bytes=VMEM_LIMIT),
        cost_estimate=pl.CostEstimate(flops=flops, bytes_accessed=64 << 20, transcendentals=0),
    )(a, at, dy, dyt, h, wg, wu, wd)


def adamw_kernel(count, sums, *refs):
    ins, outs, (g_ref, factor_ref, sem) = refs[:9], refs[9:18], refs[18:]
    blocks, _, d3, _ = sums.shape
    d = d3 // 3
    b = pl.program_id(0)

    @pl.when(b == 0)
    def _():
        def load(i):
            return pltpu.make_async_copy(sums.at[i], g_ref.at[i], sem.at[i])

        def start(i, _):
            load(i).start()
            return 0

        def square(i, total):
            load(i).wait()

            def some(k, total):
                r = pl.ds(pl.multiple_of(k * LANES, LANES), LANES)
                for half in range(2):
                    g = g_ref[i, half, r].astype(F32).reshape(LANES // 8, 8, LANES)
                    total = total + jnp.sum(g * g, axis=0)
                return total

            return lax.fori_loop(0, d3 // LANES, some, total)

        lax.fori_loop(0, blocks, start, 0)
        total = lax.fori_loop(0, blocks, square, jnp.zeros((8, LANES), F32))
        total = jnp.sum(jnp.sum(total, axis=1, keepdims=True), axis=0, keepdims=True)
        factor = jnp.minimum(1.0, 0.5 * lax.rsqrt(total / count + 1e-30))
        factor_ref[...] = jnp.broadcast_to(factor, factor_ref.shape)

    factor = factor_ref[0:1, :]
    for place in range(3):
        w_ref, m_ref, v_ref = (ins[3 * kind + place] for kind in range(3))
        w_out, m_out, v_out = (outs[3 * kind + place] for kind in range(3))
        for half in range(2):
            for k in range(0, d, LANES):
                g = g_ref[b, half, place * d + k : place * d + k + LANES, :].astype(F32)
                if place < 2:
                    at = (0, slice(k, k + LANES), slice(half * LANES, (half + 1) * LANES))
                else:
                    g = g.T
                    at = (0, slice(half * LANES, (half + 1) * LANES), slice(k, k + LANES))
                g = g * factor
                m = 0.9 * m_ref[at] + 0.1 * g
                v = 0.95 * v_ref[at] + 0.05 * g * g
                w = w_ref[at].astype(F32)
                w_out[at] = (w - 0.02 * (m * lax.rsqrt(v + 1e-8) + 0.1 * w)).astype(BF16)
                m_out[at] = m
                v_out[at] = v


def adamw(sums, arrays):
    layers, d, ff = arrays[0].shape
    per_layer = ff // BLOCK
    blocks = layers * per_layer
    wide = pl.BlockSpec((1, d, BLOCK), lambda b: (layers - 1 - b // per_layer, 0, b % per_layer))
    tall = pl.BlockSpec((1, BLOCK, d), lambda b: (layers - 1 - b // per_layer, b % per_layer, 0))
    specs = [wide, wide, tall] * 3
    return pl.pallas_call(
        functools.partial(adamw_kernel, 3 * layers * d * ff),
        grid=(blocks,),
        in_specs=[HBM] + specs,
        out_specs=specs,
        out_shape=[jax.ShapeDtypeStruct(a.shape, a.dtype) for a in arrays],
        scratch_shapes=[
            pltpu.VMEM((blocks, 2, 3 * d, LANES), BF16),
            pltpu.VMEM((8, LANES), F32),
            pltpu.SemaphoreType.DMA((blocks,)),
        ],
        compiler_params=pltpu.CompilerParams(vmem_limit_bytes=VMEM_LIMIT),
    )(sums, *arrays)


def solution(mesh):
    chips = mesh.shape["dp"] // 2

    def step(x, dy, *arrays):
        x, dy = x[0], dy[0]
        wg, wu, wd = arrays[:3]
        h, a, at, dyt = forward(x, dy, wg, wu, wd)
        sums = backward(chips, a, at, dy, dyt, h, wg, wu, wd)
        return tuple(adamw(sums, arrays))

    return jax.shard_map(
        step,
        mesh=mesh,
        in_specs=(P(("rep", "dp"), None, None),) * 2 + (P(None, None, None),) * 9,
        out_specs=(P("rep", None, None),) * 9,
        check_vma=False,
    )
```

```python
import functools

import jax
import jax.numpy as jnp
from jax import lax
from jax.experimental import pallas as pl
from jax.experimental.pallas import tpu as pltpu
from jax.sharding import PartitionSpec as P

MESH = pl.DeviceIdType.MESH
F32, BF16 = jnp.float32, jnp.bfloat16
HBM = pl.BlockSpec(memory_space=pltpu.HBM)
BLOCK = 256
LANES = 128
ROWS = 256
VMEM_LIMIT = 67_000_000


def sigmoid(x):
    return 0.5 * jnp.tanh(0.5 * x) + 0.5


def dot(a, b, contract=((1,), (0,))):
    return lax.dot_general(a, b, (contract, ((), ())), preferred_element_type=F32)


def scale_of(wide):
    return lax.rsqrt(jnp.mean(wide * wide, -1, keepdims=True) + 1e-6)


def normed(h):
    wide = h.astype(F32)
    return (wide * scale_of(wide)).astype(BF16)


def forward_kernel(x_ref, dy_ref, wg_ref, wu_ref, wd_ref, h_ref, a_ref, at_ref, dyt_ref, act_ref):
    x = x_ref[...]
    a = normed(x)
    a_ref[0] = a
    at_ref[0] = a.T
    dyt_ref[...] = dy_ref[...].T
    width = 2 * BLOCK
    for f in range(0, act_ref.shape[1], width):
        gate = dot(a, wg_ref[0, :, f : f + width])
        up = dot(a, wu_ref[0, :, f : f + width])
        act_ref[:, f : f + width] = (gate * sigmoid(gate) * up).astype(BF16)
    h = x + dot(act_ref[...], wd_ref[0]).astype(BF16)
    h_ref[...] = h
    b = normed(h)
    a_ref[1] = b
    at_ref[1] = b.T


def forward(x, dy, wg, wu, wd):
    tokens, d = x.shape
    ff = wg.shape[2]
    rows = min(512, tokens)
    tile = pl.BlockSpec((rows, d), lambda i: (i, 0))
    return pl.pallas_call(
        forward_kernel,
        grid=(tokens // rows,),
        in_specs=[tile, tile]
        + [pl.BlockSpec((1, d, ff), lambda i: (0, 0, 0))] * 2
        + [pl.BlockSpec((1, ff, d), lambda i: (0, 0, 0))],
        out_specs=[
            tile,
            pl.BlockSpec((2, rows, d), lambda i: (0, i, 0)),
            pl.BlockSpec((2, d, rows), lambda i: (0, 0, i)),
            pl.BlockSpec((d, rows), lambda i: (0, i)),
        ],
        out_shape=[
            jax.ShapeDtypeStruct((tokens, d), BF16),
            jax.ShapeDtypeStruct((2, tokens, d), BF16),
            jax.ShapeDtypeStruct((2, d, tokens), BF16),
            jax.ShapeDtypeStruct((d, tokens), BF16),
        ],
        scratch_shapes=[pltpu.VMEM((rows, ff), BF16)],
        compiler_params=pltpu.CompilerParams(vmem_limit_bytes=VMEM_LIMIT),
    )(x, dy, wg, wu, wd)


TICKS = 5
LAG = 4
DEPTH = 4


def backward_kernel(
    chips, a_hbm, at_hbm, dy_hbm, dyt_hbm, h_hbm, wg_hbm, wu_hbm, wd_hbm, sums,
    a_ref, at_ref, dy_ref, dyt_ref, h_ref, wg_ref, wu_ref, wd_ref, allg_ref, allu_ref, p_ref, dg_ref, du_ref,
    own_ref, got_ref, both_ref, land_ref,
    load_sem, w_sem, pair_send, pair_recv, rs_send, rs_recv, ag_send, ag_recv, share_send, share_recv, keep_sem,
):
    layers, tokens, d = a_hbm.shape
    ff = wg_hbm.shape[2]
    per_layer = ff // BLOCK
    blocks = layers * per_layer
    slots = blocks + layers - 1
    chunk = 3 * d // chips
    tiles = tokens // ROWS
    near = chips // 2
    far = chips - 1 - near
    inverse = next(i for i in range(TICKS) if i * LAG % TICKS == 1)

    me = lax.axis_index("dp")
    z, core = me // 2, me % 2
    other = 1 - core
    partner = {"dp": z * 2 + other}

    def wrap(c):
        return lax.rem(c + 2 * chips, chips)

    def along(step):
        return {"dp": wrap(z + step) * 2 + core}

    def rows_of(c):
        return pl.ds(pl.multiple_of(c * chunk, chunk), chunk)

    def block_of(t):
        return t - t // (per_layer + 1)

    def is_block(t):
        return (t >= 0) & (t < slots) & (lax.rem(t, per_layer + 1) != per_layer)

    def weights(b, slot):
        layer = layers - 1 - b // per_layer
        f = pl.multiple_of(lax.rem(b, per_layer) * BLOCK, BLOCK)
        return [
            pltpu.make_async_copy(wg_hbm.at[layer, :, pl.ds(f, BLOCK)], wg_ref.at[slot], w_sem.at[slot, 0]),
            pltpu.make_async_copy(wu_hbm.at[layer, :, pl.ds(f, BLOCK)], wu_ref.at[slot], w_sem.at[slot, 1]),
            pltpu.make_async_copy(wd_hbm.at[layer, pl.ds(f, BLOCK), :], wd_ref.at[slot], w_sem.at[slot, 2]),
        ]

    last = layers - 1
    loads = [
        pltpu.make_async_copy(a_hbm.at[last], a_ref, load_sem.at[0]),
        pltpu.make_async_copy(dy_hbm, dy_ref, load_sem.at[1]),
        pltpu.make_async_copy(at_hbm.at[last], at_ref, load_sem.at[2]),
        pltpu.make_async_copy(dyt_hbm, dyt_ref, load_sem.at[3]),
        pltpu.make_async_copy(wg_hbm.at[last], allg_ref, load_sem.at[4]),
        pltpu.make_async_copy(wu_hbm.at[last], allu_ref, load_sem.at[5]),
        pltpu.make_async_copy(h_hbm, h_ref, load_sem.at[6]),
        pltpu.make_async_copy(a_hbm.at[0], a_ref, load_sem.at[7]),
        pltpu.make_async_copy(at_hbm.at[0], at_ref, load_sem.at[8]),
    ]
    loads[0].start()
    for copy in weights(0, 0):
        copy.start()
    for copy in loads[1:7]:
        copy.start()

    barrier = pltpu.get_barrier_semaphore()
    for peer in (partner, along(1), along(-1)):
        pl.semaphore_signal(barrier, inc=1, device_id=peer, device_id_type=MESH)
    pl.semaphore_wait(barrier, 3)

    def pair_copy(b):
        slot = lax.rem(b, 2)
        return pltpu.make_async_remote_copy(
            own_ref.at[slot, other], got_ref.at[slot], pair_send.at[slot], pair_recv.at[slot], partner, MESH
        )

    def way_of(b, side):
        return (1 - 2 * lax.rem(b, 2)) * (1 - 2 * side)

    def rs_place(side, s):
        return side * (near + 1) + s

    def rs_copy(b, side, s):
        sem = side * near + s - 1
        return pltpu.make_async_remote_copy(
            land_ref.at[b, rs_place(side, s - 1)], land_ref.at[b, rs_place(side, s)],
            rs_send.at[b, sem], rs_recv.at[b, sem], along(way_of(b, side)), MESH,
        )

    def ag_copy(src, b, c, side, hop):
        sem = side * near + hop - 1
        return pltpu.make_async_remote_copy(
            src, sums.at[b, core, rows_of(c), :], ag_send.at[b, sem], ag_recv.at[b, sem], along(way_of(b, side)), MESH
        )

    def share_copy(src, b, c):
        return pltpu.make_async_remote_copy(src, sums.at[b, core, rows_of(c), :], share_send, share_recv, partner, MESH)

    def done(b):
        return land_ref.at[b, rs_place(0, near)]

    def keep_copy(b):
        return pltpu.make_async_copy(done(b), sums.at[b, core, rows_of(z), :], keep_sem.at[b])

    def scatter_step(b, s):
        four = lax.rem(b, DEPTH)

        @pl.when(s == 1)
        def _():
            slot = lax.rem(b, 2)
            pair_copy(b).wait()

            def add(i, _):
                r = rows_of(i)
                both_ref[four, r] = own_ref[slot, core, r].astype(F32) + got_ref[slot, r].astype(F32)
                return 0

            lax.fori_loop(0, chips, add, 0)
            for side, reach in ((0, near), (1, far)):
                c = wrap(z + way_of(b, side) * reach)
                land_ref[b, rs_place(side, 0)] = both_ref[four, rows_of(c)].astype(BF16)

        for side, reach in ((0, near), (1, far)):

            @pl.when((s > 1) & (s <= reach))
            def _(side=side, reach=reach):
                rs_copy(b, side, s - 1).wait_recv()
                here = rs_place(side, s - 1)
                c = wrap(z + way_of(b, side) * (reach + 1 - s))
                land_ref[b, here] = (land_ref[b, here].astype(F32) + both_ref[four, rows_of(c)]).astype(BF16)

        @pl.when(s == near + 1)
        def _():
            rs_copy(b, 0, near).wait_recv()
            rs_copy(b, 1, far).wait_recv()
            total = both_ref[four, rows_of(z)] + land_ref[b, rs_place(1, far)].astype(F32)
            land_ref[b, rs_place(0, near)] = (total + land_ref[b, rs_place(0, near)].astype(F32)).astype(BF16)

        for side, reach in ((0, near), (1, far)):

            @pl.when(s <= reach)
            def _(side=side):
                rs_copy(b, side, s).start()

        @pl.when(s == near + 1)
        def _():
            for side in range(2):
                ag_copy(done(b), b, z, side, 1).start()
            share_copy(done(b), b, z).start()
            keep_copy(b).start()

    def gather_step(b, hop):
        for side, reach in ((0, near), (1, far)):

            @pl.when(hop <= reach)
            def _(side=side, reach=reach):
                c = wrap(z - way_of(b, side) * hop)
                here = sums.at[b, core, rows_of(c), :]
                ag_copy(here, b, c, side, hop).wait_recv()

                @pl.when(hop < reach)
                def _():
                    ag_copy(here, b, c, side, hop + 1).start()

                share_copy(here, b, c).start()

    def tick(now):
        first = lax.rem(inverse * now, TICKS)
        for p, step in ((first, scatter_step), (first + TICKS, gather_step)):
            t = (now - LAG * p + 16 * TICKS) // TICKS - 17
            ok = is_block(t)
            if step is gather_step:
                ok = ok & (p < near + 1 + near)

            @pl.when(ok)
            def _(t=t, step=step):
                step(block_of(t), first + 1)

    def token_tiles(slot, kept, first, count):
        for i in range(count):
            r = pl.ds(pl.multiple_of((first + i) * ROWS, ROWS), ROWS)
            a = a_ref[r]
            gate, up = dot(a, wg_ref[slot]), dot(a, wu_ref[slot])
            by_p = dot(dy_ref[r], wd_ref[slot], ((1,), (1,))).astype(BF16).astype(F32)
            s = sigmoid(gate)
            silu = gate * s
            p_ref[r] = (silu * up).astype(BF16)
            du_ref[kept, r] = (by_p * silu).astype(BF16)
            dg_ref[kept, r] = (by_p * up * (s + silu * (1.0 - s))).astype(BF16)

    def next_layer(first, count):
        for i in range(count):
            r = pl.ds(pl.multiple_of((first + i) * ROWS, ROWS), ROWS)
            wide = h_ref[r].astype(F32)

            def through(by_ref, w_ref):
                total = jnp.zeros((ROWS, d), F32)
                for k in range(per_layer):
                    total = total + dot(by_ref[k, r], w_ref[:, k * BLOCK : (k + 1) * BLOCK], ((1,), (1,)))
                return total.astype(BF16).astype(F32)

            by_a = (through(dg_ref, allg_ref) + through(du_ref, allu_ref)).astype(BF16).astype(F32)
            scale = scale_of(wide)
            inner = jnp.sum(by_a * wide, -1, keepdims=True) * (scale * scale * scale / d)
            by_h = dy_ref[r] + (by_a * scale - wide * inner).astype(BF16)
            dy_ref[r] = by_h
            dyt_ref[:, r] = by_h.T

    parts = TICKS - 1
    each = tiles // parts

    def slot_of_work(t, _):
        @pl.when(is_block(t))
        def _():
            b = block_of(t)
            slot = lax.rem(b, 2)
            kept = lax.rem(b, per_layer)

            @pl.when(b + 1 < blocks)
            def _():
                for copy in weights(b + 1, 1 - slot):
                    copy.start()

            @pl.when(t == 0)
            def _():
                loads[0].wait()
                loads[1].wait()

            for copy in weights(b, slot):
                copy.wait()

            def part(i, _):
                token_tiles(slot, kept, i * each, each)
                tick(TICKS * t + i)
                return 0

            lax.fori_loop(0, parts, part, 0)

            @pl.when(t == 0)
            def _():
                loads[2].wait()
                loads[3].wait()

            for place, (left, right) in enumerate(
                ((at_ref, dg_ref.at[kept]), (at_ref, du_ref.at[kept]), (dyt_ref, p_ref))
            ):
                g = dot(left[...], right[...]).astype(BF16)
                for half in range(2):
                    own_ref[slot, half, place * d : (place + 1) * d, :] = g[:, half * LANES : (half + 1) * LANES]
            pair_copy(b).start()
            tick(TICKS * t + parts)

        @pl.when(jnp.logical_not(is_block(t)))
        def _():
            for copy in loads[7:]:
                copy.start()
            for copy in loads[4:7]:
                copy.wait()

            def part(i, _):
                next_layer(i * each, each)
                tick(TICKS * t + i)
                return 0

            lax.fori_loop(0, parts, part, 0)
            tick(TICKS * t + parts)
            for copy in loads[7:]:
                copy.wait()

        return 0

    lax.fori_loop(0, slots, slot_of_work, 0)

    def drain(now, _):
        tick(now)
        return 0

    lax.fori_loop(TICKS * slots, TICKS * slots + LAG * 2 * near + 1, drain, 0)

    def finish(b, _):
        for side, reach in ((0, near), (1, far)):
            for hop in range(1, reach + 1):
                rs_copy(b, side, hop).wait_send()
                ag_copy(done(b), b, z, side, hop).wait_send()
        keep_copy(b).wait()
        return 0

    lax.fori_loop(0, blocks, finish, 0)
    pltpu.make_async_copy(sums.at[:, core], sums.at[:, core], share_send).wait()
    pltpu.make_async_copy(sums.at[:, other], sums.at[:, other], share_recv).wait()


def backward(chips, a, at, dy, dyt, h, wg, wu, wd):
    layers, tokens, d = a.shape
    ff = wg.shape[2]
    per_layer = ff // BLOCK
    blocks = layers * per_layer
    chunk = 3 * d // chips
    vmem = pltpu.VMEM
    sem = pltpu.SemaphoreType.DMA
    flops = 2 * tokens * d * ff * (6 * layers + 2)
    return pl.pallas_call(
        functools.partial(backward_kernel, chips),
        out_shape=jax.ShapeDtypeStruct((blocks, 2, 3 * d, LANES), BF16),
        in_specs=[HBM] * 8,
        out_specs=HBM,
        scratch_shapes=[
            vmem((tokens, d), BF16), vmem((d, tokens), BF16), vmem((tokens, d), BF16), vmem((d, tokens), BF16),
            vmem((tokens, d), BF16), vmem((2, d, BLOCK), BF16), vmem((2, d, BLOCK), BF16), vmem((2, BLOCK, d), BF16),
            vmem((d, ff), BF16), vmem((d, ff), BF16),
            vmem((tokens, BLOCK), BF16), vmem((per_layer, tokens, BLOCK), BF16), vmem((per_layer, tokens, BLOCK), BF16),
            vmem((2, 2, 3 * d, LANES), BF16), vmem((2, 3 * d, LANES), BF16), vmem((DEPTH, 3 * d, LANES), F32),
            vmem((blocks, chips + 1, chunk, LANES), BF16),
            sem((9,)), sem((2, 3)), sem((2,)), sem((2,)), sem((blocks, chips - 1)), sem((blocks, chips - 1)),
            sem((blocks, chips - 1)), sem((blocks, chips - 1)), sem, sem, sem((blocks,)),
        ],
        compiler_params=pltpu.CompilerParams(collective_id=0, has_side_effects=True, vmem_limit_bytes=VMEM_LIMIT),
        cost_estimate=pl.CostEstimate(flops=flops, bytes_accessed=64 << 20, transcendentals=0),
    )(a, at, dy, dyt, h, wg, wu, wd)


def adamw_kernel(count, sums, *refs):
    ins, outs, (g_ref, factor_ref, sem) = refs[:9], refs[9:18], refs[18:]
    blocks, _, d3, _ = sums.shape
    d = d3 // 3
    b = pl.program_id(0)

    @pl.when(b == 0)
    def _():
        def load(i):
            return pltpu.make_async_copy(sums.at[i], g_ref.at[i], sem.at[i])

        def start(i, _):
            load(i).start()
            return 0

        def square(i, total):
            load(i).wait()

            def some(k, total):
                r = pl.ds(pl.multiple_of(k * LANES, LANES), LANES)
                for half in range(2):
                    g = g_ref[i, half, r].astype(F32).reshape(LANES // 8, 8, LANES)
                    total = total + jnp.sum(g * g, axis=0)
                return total

            return lax.fori_loop(0, d3 // LANES, some, total)

        lax.fori_loop(0, blocks, start, 0)
        total = lax.fori_loop(0, blocks, square, jnp.zeros((8, LANES), F32))
        total = jnp.sum(jnp.sum(total, axis=1, keepdims=True), axis=0, keepdims=True)
        factor = jnp.minimum(1.0, 0.5 * lax.rsqrt(total / count + 1e-30))
        factor_ref[...] = jnp.broadcast_to(factor, factor_ref.shape)

    factor = factor_ref[0:1, :]
    for place in range(3):
        w_ref, m_ref, v_ref = (ins[3 * kind + place] for kind in range(3))
        w_out, m_out, v_out = (outs[3 * kind + place] for kind in range(3))
        for half in range(2):
            for k in range(0, d, LANES):
                g = g_ref[b, half, place * d + k : place * d + k + LANES, :].astype(F32)
                if place < 2:
                    at = (0, slice(k, k + LANES), slice(half * LANES, (half + 1) * LANES))
                else:
                    g = g.T
                    at = (0, slice(half * LANES, (half + 1) * LANES), slice(k, k + LANES))
                g = g * factor
                m = 0.9 * m_ref[at] + 0.1 * g
                v = 0.95 * v_ref[at] + 0.05 * g * g
                w = w_ref[at].astype(F32)
                w_out[at] = (w - 0.02 * (m * lax.rsqrt(v + 1e-8) + 0.1 * w)).astype(BF16)
                m_out[at] = m
                v_out[at] = v


def adamw(sums, arrays):
    layers, d, ff = arrays[0].shape
    per_layer = ff // BLOCK
    blocks = layers * per_layer
    wide = pl.BlockSpec((1, d, BLOCK), lambda b: (layers - 1 - b // per_layer, 0, b % per_layer))
    tall = pl.BlockSpec((1, BLOCK, d), lambda b: (layers - 1 - b // per_layer, b % per_layer, 0))
    specs = [wide, wide, tall] * 3
    return pl.pallas_call(
        functools.partial(adamw_kernel, 3 * layers * d * ff),
        grid=(blocks,),
        in_specs=[HBM] + specs,
        out_specs=specs,
        out_shape=[jax.ShapeDtypeStruct(a.shape, a.dtype) for a in arrays],
        scratch_shapes=[
            pltpu.VMEM((blocks, 2, 3 * d, LANES), BF16),
            pltpu.VMEM((8, LANES), F32),
            pltpu.SemaphoreType.DMA((blocks,)),
        ],
        compiler_params=pltpu.CompilerParams(vmem_limit_bytes=VMEM_LIMIT),
    )(sums, *arrays)


def solution(mesh):
    chips = mesh.shape["dp"] // 2

    def step(x, dy, *arrays):
        x, dy = x[0], dy[0]
        wg, wu, wd = arrays[:3]
        h, a, at, dyt = forward(x, dy, wg, wu, wd)
        sums = backward(chips, a, at, dy, dyt, h, wg, wu, wd)
        return tuple(adamw(sums, arrays))

    return jax.shard_map(
        step,
        mesh=mesh,
        in_specs=(P(("rep", "dp"), None, None),) * 2 + (P(None, None, None),) * 9,
        out_specs=(P("rep", None, None),) * 9,
        check_vma=False,
    )
```

```python
import functools

import jax
import jax.numpy as jnp
from jax import lax
from jax.experimental import pallas as pl
from jax.experimental.pallas import tpu as pltpu
from jax.sharding import PartitionSpec as P

MESH = pl.DeviceIdType.MESH
F32, BF16 = jnp.float32, jnp.bfloat16
HBM = pl.BlockSpec(memory_space=pltpu.HBM)
BLOCK = 256
LANES = 128
ROWS = 256
WIDE = 2
VMEM_LIMIT = 67_000_000


def sigmoid(x):
    return 0.5 * jnp.tanh(0.5 * x) + 0.5


def dot(a, b, contract=((1,), (0,))):
    return lax.dot_general(a, b, (contract, ((), ())), preferred_element_type=F32)


def scale_of(wide):
    return lax.rsqrt(jnp.mean(wide * wide, -1, keepdims=True) + 1e-6)


def normed(h):
    wide = h.astype(F32)
    return (wide * scale_of(wide)).astype(BF16)


def forward_kernel(x_ref, dy_ref, wg_ref, wu_ref, wd_ref, h_ref, a_ref, at_ref, dyt_ref, act_ref):
    x = x_ref[...]
    a = normed(x)
    a_ref[0] = a
    at_ref[0] = a.T
    dyt_ref[...] = dy_ref[...].T
    width = 2 * BLOCK
    for f in range(0, act_ref.shape[1], width):
        gate = dot(a, wg_ref[0, :, f : f + width])
        up = dot(a, wu_ref[0, :, f : f + width])
        act_ref[:, f : f + width] = (gate * sigmoid(gate) * up).astype(BF16)
    h = x + dot(act_ref[...], wd_ref[0]).astype(BF16)
    h_ref[...] = h
    b = normed(h)
    a_ref[1] = b
    at_ref[1] = b.T


def forward(x, dy, wg, wu, wd):
    tokens, d = x.shape
    ff = wg.shape[2]
    rows = min(512, tokens)
    tile = pl.BlockSpec((rows, d), lambda i: (i, 0))
    return pl.pallas_call(
        forward_kernel,
        grid=(tokens // rows,),
        in_specs=[tile, tile]
        + [pl.BlockSpec((1, d, ff), lambda i: (0, 0, 0))] * 2
        + [pl.BlockSpec((1, ff, d), lambda i: (0, 0, 0))],
        out_specs=[
            tile,
            pl.BlockSpec((2, rows, d), lambda i: (0, i, 0)),
            pl.BlockSpec((2, d, rows), lambda i: (0, 0, i)),
            pl.BlockSpec((d, rows), lambda i: (0, i)),
        ],
        out_shape=[
            jax.ShapeDtypeStruct((tokens, d), BF16),
            jax.ShapeDtypeStruct((2, tokens, d), BF16),
            jax.ShapeDtypeStruct((2, d, tokens), BF16),
            jax.ShapeDtypeStruct((d, tokens), BF16),
        ],
        scratch_shapes=[pltpu.VMEM((rows, ff), BF16)],
        compiler_params=pltpu.CompilerParams(vmem_limit_bytes=VMEM_LIMIT),
    )(x, dy, wg, wu, wd)


PARTS = 4
TICKS = PARTS + 1
LAG = 4
DEPTH = 4


def backward_kernel(
    chips, a_hbm, at_hbm, dy_hbm, dyt_hbm, h_hbm, wg_hbm, wu_hbm, wd_hbm, sums,
    a_ref, at_ref, dy_ref, dyt_ref, h_ref, wg_ref, wu_ref, wd_ref, allg_ref, allu_ref, p_ref, dg_ref, du_ref,
    own_ref, got_ref, both_ref, land_ref, spread_ref,
    load_sem, w_sem, pair_send, pair_recv, rs_send, rs_recv, ag_send, ag_recv, share_send, share_recv, keep_sem,
):
    layers, tokens, d = a_hbm.shape
    ff = wg_hbm.shape[2]
    per_layer = ff // BLOCK
    blocks = layers * per_layer
    slots = blocks + layers - 1
    chunk = 3 * d // chips
    tiles = tokens // ROWS
    near = chips // 2
    far = chips - 1 - near
    inverse = next(i for i in range(TICKS) if i * LAG % TICKS == 1)

    me = lax.axis_index("dp")
    z, core = me // 2, me % 2
    other = 1 - core
    partner = {"dp": z * 2 + other}

    def wrap(c):
        return lax.rem(c + 2 * chips, chips)

    def along(step):
        return {"dp": wrap(z + step) * 2 + core}

    def rows_of(c):
        return pl.ds(pl.multiple_of(c * chunk, chunk), chunk)

    def block_of(t):
        return t - t // (per_layer + 1)

    def is_block(t):
        return (t >= 0) & (t < slots) & (lax.rem(t, per_layer + 1) != per_layer)

    def weights(b, slot):
        layer = layers - 1 - b // per_layer
        f = pl.multiple_of(lax.rem(b, per_layer) * BLOCK, BLOCK)
        return [
            pltpu.make_async_copy(wg_hbm.at[layer, :, pl.ds(f, BLOCK)], wg_ref.at[slot], w_sem.at[slot, 0]),
            pltpu.make_async_copy(wu_hbm.at[layer, :, pl.ds(f, BLOCK)], wu_ref.at[slot], w_sem.at[slot, 1]),
            pltpu.make_async_copy(wd_hbm.at[layer, pl.ds(f, BLOCK), :], wd_ref.at[slot], w_sem.at[slot, 2]),
        ]

    last = layers - 1
    loads = [
        pltpu.make_async_copy(a_hbm.at[last], a_ref, load_sem.at[0]),
        pltpu.make_async_copy(dy_hbm, dy_ref, load_sem.at[1]),
        pltpu.make_async_copy(at_hbm.at[last], at_ref, load_sem.at[2]),
        pltpu.make_async_copy(dyt_hbm, dyt_ref, load_sem.at[3]),
        pltpu.make_async_copy(wg_hbm.at[last], allg_ref, load_sem.at[4]),
        pltpu.make_async_copy(wu_hbm.at[last], allu_ref, load_sem.at[5]),
        pltpu.make_async_copy(h_hbm, h_ref, load_sem.at[6]),
        pltpu.make_async_copy(a_hbm.at[0], a_ref, load_sem.at[7]),
        pltpu.make_async_copy(at_hbm.at[0], at_ref, load_sem.at[8]),
    ]
    loads[0].start()
    for copy in weights(0, 0):
        copy.start()
    loads[1].start()

    barrier = pltpu.get_barrier_semaphore()
    for peer in (partner, along(1), along(-1)):
        pl.semaphore_signal(barrier, inc=1, device_id=peer, device_id_type=MESH)
    pl.semaphore_wait(barrier, 3)

    def pair_copy(b):
        slot = lax.rem(b, 2)
        return pltpu.make_async_remote_copy(
            own_ref.at[slot, other], got_ref.at[slot], pair_send.at[slot], pair_recv.at[slot], partner, MESH
        )

    def way_of(b, side):
        return (1 - 2 * lax.rem(b, 2)) * (1 - 2 * side)

    def rs_place(side, s):
        return side * (near + 1) + s

    def rs_copy(b, side, s):
        sem = side * near + s - 1
        return pltpu.make_async_remote_copy(
            land_ref.at[b, rs_place(side, s - 1)], land_ref.at[b, rs_place(side, s)],
            rs_send.at[b, sem], rs_recv.at[b, sem], along(way_of(b, side)), MESH,
        )

    def ag_copy(src, b, side, hop):
        place = side * near + hop - 1
        return pltpu.make_async_remote_copy(
            src, spread_ref.at[b, place], ag_send.at[b, place], ag_recv.at[b, place], along(way_of(b, 1 - side)), MESH
        )

    def share_copy(src, b, c):
        return pltpu.make_async_remote_copy(src, sums.at[b, core, rows_of(c), :], share_send, share_recv, partner, MESH)

    def keep_copy(src, b, c):
        return pltpu.make_async_copy(src, sums.at[b, core, rows_of(c), :], keep_sem)

    def done(b):
        return land_ref.at[b, rs_place(0, near)]

    def scatter_step(b, s):
        four = lax.rem(b, DEPTH)

        @pl.when(s == 1)
        def _():
            slot = lax.rem(b, 2)
            pair_copy(b).wait()

            def add(i, _):
                r = rows_of(i)
                both_ref[four, r] = own_ref[slot, core, r].astype(F32) + got_ref[slot, r].astype(F32)
                return 0

            lax.fori_loop(0, chips, add, 0)
            for side, reach in ((0, near), (1, far)):
                c = wrap(z + way_of(b, side) * reach)
                land_ref[b, rs_place(side, 0)] = both_ref[four, rows_of(c)].astype(BF16)

        for side, reach in ((0, near), (1, far)):

            @pl.when((s > 1) & (s <= reach))
            def _(side=side, reach=reach):
                rs_copy(b, side, s - 1).wait_recv()
                here = rs_place(side, s - 1)
                c = wrap(z + way_of(b, side) * (reach + 1 - s))
                land_ref[b, here] = (land_ref[b, here].astype(F32) + both_ref[four, rows_of(c)]).astype(BF16)

        @pl.when(s == near + 1)
        def _():
            rs_copy(b, 0, near).wait_recv()
            rs_copy(b, 1, far).wait_recv()
            total = both_ref[four, rows_of(z)] + land_ref[b, rs_place(1, far)].astype(F32)
            land_ref[b, rs_place(0, near)] = (total + land_ref[b, rs_place(0, near)].astype(F32)).astype(BF16)

        for side, reach in ((0, near), (1, far)):

            @pl.when(s <= reach)
            def _(side=side):
                rs_copy(b, side, s).start()

        @pl.when(s == near + 1)
        def _():
            for side in range(2):
                ag_copy(done(b), b, side, 1).start()
            share_copy(done(b), b, z).start()
            keep_copy(done(b), b, z).start()

    def gather_step(b, hop):
        for side, reach in ((0, near), (1, far)):

            @pl.when(hop <= reach)
            def _(side=side, reach=reach):
                c = wrap(z - way_of(b, 1 - side) * hop)
                here = spread_ref.at[b, side * near + hop - 1]
                ag_copy(here, b, side, hop).wait_recv()

                @pl.when(hop < reach)
                def _():
                    ag_copy(here, b, side, hop + 1).start()

                share_copy(here, b, c).start()
                keep_copy(here, b, c).start()

    def tick(now):
        first = lax.rem(inverse * now, TICKS)
        later = jnp.where(first > near, first, first + TICKS)
        for p, step, phase in ((later, gather_step, later - near), (first, scatter_step, first + 1)):
            t = (now - LAG * p + 16 * TICKS) // TICKS - 17

            @pl.when(is_block(t) & (phase <= (near + 1 if step is scatter_step else near)))
            def _(t=t, step=step, phase=phase):
                step(block_of(t), phase)

    def token_tiles(slot, kept, first, count):
        for i in range(count):
            r = pl.ds(pl.multiple_of((first + i) * ROWS, ROWS), ROWS)
            a = a_ref[r]
            gate, up = dot(a, wg_ref[slot]), dot(a, wu_ref[slot])
            by_p = dot(dy_ref[r], wd_ref[slot], ((1,), (1,))).astype(BF16).astype(F32)
            s = sigmoid(gate)
            silu = gate * s
            p_ref[r] = (silu * up).astype(BF16)
            du_ref[kept, r] = (by_p * silu).astype(BF16)
            dg_ref[kept, r] = (by_p * up * (s + silu * (1.0 - s))).astype(BF16)

    def next_layer(first, count):
        for i in range(count):
            r = pl.ds(pl.multiple_of((first + i) * ROWS, ROWS), ROWS)
            wide = h_ref[r].astype(F32)

            def through(by_ref, w_ref):
                total = jnp.zeros((ROWS, d), F32)
                for k in range(per_layer):
                    total = total + dot(by_ref[k, r], w_ref[:, k * BLOCK : (k + 1) * BLOCK], ((1,), (1,)))
                return total.astype(BF16).astype(F32)

            by_a = (through(dg_ref, allg_ref) + through(du_ref, allu_ref)).astype(BF16).astype(F32)
            scale = scale_of(wide)
            inner = jnp.sum(by_a * wide, -1, keepdims=True) * (scale * scale * scale / d)
            by_h = dy_ref[r] + (by_a * scale - wide * inner).astype(BF16)
            dy_ref[r] = by_h
            dyt_ref[:, r] = by_h.T

    parts = PARTS
    each = tiles // parts

    def slot_of_work(t, _):
        @pl.when(is_block(t))
        def _():
            b = block_of(t)
            slot = lax.rem(b, 2)
            kept = lax.rem(b, per_layer)

            @pl.when(b + 1 < blocks)
            def _():
                for copy in weights(b + 1, 1 - slot):
                    copy.start()

            @pl.when(t == 0)
            def _():
                loads[0].wait()
                loads[1].wait()
                loads[2].start()
                loads[3].start()

            @pl.when(t == 1)
            def _():
                for copy in loads[4:7]:
                    copy.start()

            for copy in weights(b, slot):
                copy.wait()

            def part(i, _):
                token_tiles(slot, kept, i * each, each)
                tick(TICKS * t + i)
                return 0

            lax.fori_loop(0, parts, part, 0)

            @pl.when(t == 0)
            def _():
                loads[2].wait()
                loads[3].wait()

            for place, (left, right) in enumerate(
                ((at_ref, dg_ref.at[kept]), (at_ref, du_ref.at[kept]), (dyt_ref, p_ref))
            ):
                g = dot(left[...], right[...]).astype(BF16)
                for half in range(2):
                    own_ref[slot, half, place * d : (place + 1) * d, :] = g[:, half * LANES : (half + 1) * LANES]
            pair_copy(b).start()
            tick(TICKS * t + TICKS - 1)

        @pl.when(jnp.logical_not(is_block(t)))
        def _():
            for copy in loads[7:]:
                copy.start()
            for copy in loads[4:7]:
                copy.wait()

            def part(i, _):
                next_layer(i * each, each)
                tick(TICKS * t + i)
                return 0

            lax.fori_loop(0, parts, part, 0)
            for i in range(parts, TICKS):
                tick(TICKS * t + i)
            for copy in loads[7:]:
                copy.wait()

        return 0

    lax.fori_loop(0, slots, slot_of_work, 0)

    def drain(now, _):
        tick(now)
        return 0

    lax.fori_loop(TICKS * slots, TICKS * slots + LAG * 2 * near + 1, drain, 0)

    def finish(b, _):
        for side, reach in ((0, near), (1, far)):
            for hop in range(1, reach + 1):
                rs_copy(b, side, hop).wait_send()
                ag_copy(done(b), b, side, hop).wait_send()
        return 0

    lax.fori_loop(0, blocks, finish, 0)
    pltpu.make_async_copy(sums.at[:, core], sums.at[:, core], keep_sem).wait()
    pltpu.make_async_copy(sums.at[:, core], sums.at[:, core], share_send).wait()
    pltpu.make_async_copy(sums.at[:, other], sums.at[:, other], share_recv).wait()


def backward(chips, a, at, dy, dyt, h, wg, wu, wd):
    layers, tokens, d = a.shape
    ff = wg.shape[2]
    per_layer = ff // BLOCK
    blocks = layers * per_layer
    chunk = 3 * d // chips
    vmem = pltpu.VMEM
    sem = pltpu.SemaphoreType.DMA
    flops = 2 * tokens * d * ff * (6 * layers + 2)
    return pl.pallas_call(
        functools.partial(backward_kernel, chips),
        out_shape=jax.ShapeDtypeStruct((blocks, 2, 3 * d, LANES), BF16),
        in_specs=[HBM] * 8,
        out_specs=HBM,
        scratch_shapes=[
            vmem((tokens, d), BF16), vmem((d, tokens), BF16), vmem((tokens, d), BF16), vmem((d, tokens), BF16),
            vmem((tokens, d), BF16), vmem((2, d, BLOCK), BF16), vmem((2, d, BLOCK), BF16), vmem((2, BLOCK, d), BF16),
            vmem((d, ff), BF16), vmem((d, ff), BF16),
            vmem((tokens, BLOCK), BF16), vmem((per_layer, tokens, BLOCK), BF16), vmem((per_layer, tokens, BLOCK), BF16),
            vmem((2, 2, 3 * d, LANES), BF16), vmem((2, 3 * d, LANES), BF16), vmem((DEPTH, 3 * d, LANES), F32),
            vmem((blocks, chips + 1, chunk, LANES), BF16), vmem((blocks, chips - 1, chunk, LANES), BF16),
            sem((9,)), sem((2, 3)), sem((2,)), sem((2,)), sem((blocks, chips - 1)), sem((blocks, chips - 1)),
            sem((blocks, chips - 1)), sem((blocks, chips - 1)), sem, sem, sem,
        ],
        compiler_params=pltpu.CompilerParams(collective_id=0, has_side_effects=True, vmem_limit_bytes=VMEM_LIMIT),
        cost_estimate=pl.CostEstimate(flops=flops, bytes_accessed=64 << 20, transcendentals=0),
    )(a, at, dy, dyt, h, wg, wu, wd)


def adamw_kernel(count, sums, *refs):
    ins, outs, (g_ref, factor_ref, sem) = refs[:9], refs[9:18], refs[18:]
    blocks, _, d3, _ = sums.shape
    d = d3 // 3
    step = pl.program_id(0)

    @pl.when(step == 0)
    def _():
        def load(i):
            return pltpu.make_async_copy(sums.at[i], g_ref.at[i], sem.at[i])

        def start(i, _):
            load(i).start()
            return 0

        def square(i, total):
            load(i).wait()

            def some(k, total):
                r = pl.ds(pl.multiple_of(k * LANES, LANES), LANES)
                for half in range(2):
                    g = g_ref[i, half, r].astype(F32).reshape(LANES // 8, 8, LANES)
                    total = total + jnp.sum(g * g, axis=0)
                return total

            return lax.fori_loop(0, d3 // LANES, some, total)

        lax.fori_loop(0, blocks, start, 0)
        total = lax.fori_loop(0, blocks, square, jnp.zeros((8, LANES), F32))
        total = jnp.sum(jnp.sum(total, axis=1, keepdims=True), axis=0, keepdims=True)
        factor = jnp.minimum(1.0, 0.5 * lax.rsqrt(total / count + 1e-30))
        factor_ref[...] = jnp.broadcast_to(factor, factor_ref.shape)

    factor = factor_ref[0:1, :]
    for sub in range(2 * WIDE):
        start, half = sub * LANES, sub % 2
        block = step * WIDE + sub // 2
        for place in range(3):
            w_ref, m_ref, v_ref = (ins[3 * kind + place] for kind in range(3))
            w_out, m_out, v_out = (outs[3 * kind + place] for kind in range(3))
            for k in range(0, d, LANES):
                g = g_ref[block, half, place * d + k : place * d + k + LANES, :].astype(F32)
                if place < 2:
                    at = (0, slice(k, k + LANES), slice(start, start + LANES))
                else:
                    g = g.T
                    at = (0, slice(start, start + LANES), slice(k, k + LANES))
                g = g * factor
                m = 0.9 * m_ref[at] + 0.1 * g
                v = 0.95 * v_ref[at] + 0.05 * g * g
                w = w_ref[at].astype(F32)
                w_out[at] = (w - 0.02 * (m * lax.rsqrt(v + 1e-8) + 0.1 * w)).astype(BF16)
                m_out[at] = m
                v_out[at] = v


def adamw(sums, arrays):
    layers, d, ff = arrays[0].shape
    per_layer = ff // BLOCK
    blocks = layers * per_layer
    steps = per_layer // WIDE
    wide = pl.BlockSpec((1, d, WIDE * BLOCK), lambda i: (layers - 1 - i // steps, 0, i % steps))
    tall = pl.BlockSpec((1, WIDE * BLOCK, d), lambda i: (layers - 1 - i // steps, i % steps, 0))
    specs = [wide, wide, tall] * 3
    return pl.pallas_call(
        functools.partial(adamw_kernel, 3 * layers * d * ff),
        grid=(layers * steps,),
        in_specs=[HBM] + specs,
        out_specs=specs,
        out_shape=[jax.ShapeDtypeStruct(a.shape, a.dtype) for a in arrays],
        scratch_shapes=[
            pltpu.VMEM((blocks, 2, 3 * d, LANES), BF16),
            pltpu.VMEM((8, LANES), F32),
            pltpu.SemaphoreType.DMA((blocks,)),
        ],
        compiler_params=pltpu.CompilerParams(vmem_limit_bytes=VMEM_LIMIT),
    )(sums, *arrays)


def solution(mesh):
    chips = mesh.shape["dp"] // 2

    def step(x, dy, *arrays):
        x, dy = x[0], dy[0]
        wg, wu, wd = arrays[:3]
        h, a, at, dyt = forward(x, dy, wg, wu, wd)
        sums = backward(chips, a, at, dy, dyt, h, wg, wu, wd)
        return tuple(adamw(sums, arrays))

    return jax.shard_map(
        step,
        mesh=mesh,
        in_specs=(P(("rep", "dp"), None, None),) * 2 + (P(None, None, None),) * 9,
        out_specs=(P("rep", None, None),) * 9,
        check_vma=False,
    )
```
